128 devices in a mesh: grp: 8 (over y_hi, z), pair: 16 (over x, y_lo, core).
Axes of the slice: x: 4, y: 4 (y_hi: 2, y_lo: 2; y = y_hi * 2 + y_lo), z: 4, core: 2. Of those that a mesh axis runs over, the one named last changes fastest.
Arguments:
- amplitudes: bfloat16 [128, 512, 512], P('pair', 'grp'), may hold values from -6 to 6
- cholesky: bfloat16 [512, 512, 2048], P('pair', 'grp'), may hold values from -0.09375 to 0.09375
Outputs:
- ladder_term: float32 [512, 4, 128], P('pair', None, 'grp')
The draws below stay inside these ranges and needn't reach their ends.
All inputs are finite; a program needn't handle non-finite values.
Results may differ from the reference program's by a relative error of at most 0.003.
Values may be sent and summed in bfloat16 or wider, within the bound.
A program may use at most 128 MiB of HBM per device.

```python
import jax
import jax.numpy as jnp
from jax import lax

VIRT = 512
NAUX = 2048
A_WIN = 4
NPAIR = 128


def levels(own_key, shape, shards, low, high):
    loudness = 1.0
    for axis_at, shards_of in shards:
        draws = jax.random.uniform(jax.random.fold_in(jax.random.fold_in(own_key, 6), axis_at), (shards_of,), jnp.float32, low / len(shards), high / len(shards))
        loudness = loudness * jnp.repeat(jnp.exp(draws), shape[axis_at] // shards_of).reshape((-1,) + (1,) * (len(shape) - 1 - axis_at))
    return loudness


def bell_draw(own_key, dims, spread, bound, split=(), kind=jnp.bfloat16):
    entries = jax.random.normal(own_key, dims, jnp.float32) * spread
    if len(split) > 0:
        entries = levels(own_key, dims, split, -0.22, 0.18) * entries
    return jnp.clip(entries, min=-bound, max=bound).astype(kind)


def setup_inputs(seed: int = 0) -> dict:
    splits = jax.random.split(jax.random.key(seed), 3)
    amplitudes = bell_draw(splits[0], (NPAIR, VIRT, VIRT), 1.0, 6.0, ((0, 16), (1, 8)))
    cholesky = bell_draw(splits[1], (VIRT, VIRT, NAUX), ((VIRT * VIRT * NAUX) ** -0.25), 0.09375, ((0, 16), (1, 8)))
    return {"amplitudes": amplitudes, "cholesky": cholesky}


def reference(amplitudes, cholesky):
    tiles_count = 8
    tile_width = VIRT // tiles_count
    window_chol = cholesky[:A_WIN]
    flat_chol = cholesky.reshape(VIRT * VIRT, NAUX)

    def one_tile(running, tile_index):
        offset = (tile_index * tile_width).astype(jnp.int32)
        portion = lax.dynamic_slice_in_dim(window_chol, offset, tile_width, 1)
        product = lax.dot_general(flat_chol, portion.reshape(A_WIN * tile_width, NAUX), (((1,), (1,)), ((), ())), preferred_element_type=jnp.float32)
        integrals = product.astype(jnp.bfloat16).reshape(VIRT, VIRT, A_WIN, tile_width)
        amp_slice = lax.dynamic_slice_in_dim(amplitudes, offset, tile_width, 2)
        contrib = lax.dot_general(integrals, amp_slice, (((1, 3), (1, 2)), ((), ())), preferred_element_type=jnp.float32)
        return running + contrib, None

    initial = jnp.zeros((VIRT, A_WIN, NPAIR), jnp.float32)
    result, unused = lax.scan(one_tile, initial, jnp.arange(tiles_count, dtype=jnp.int32))
    return result
```

```python
import jax
import jax.numpy as jnp
from jax import lax
from jax.experimental import pallas as pl
from jax.experimental.pallas import tpu as pltpu
from jax.sharding import PartitionSpec as P

A_WIN = 4
MESH = pl.DeviceIdType.MESH
F32, BF16 = jnp.float32, jnp.bfloat16


ROW_CHUNK = 1024
X_OF_PIECE = (0, 1, 0, 3)
ROW_PLAN = (
    ((0, (1, 0)), (2, (1, 0)), (1, (0,)), (3, (1,))),
    ((1, (0, 1)), (0, (1,)), (2, ()), (3, ())),
    ((0, ()), (1, ()), (2, ()), (3, ())),
    ((3, (1, 0)), (2, (0,)), (0, ()), (1, ())),
)


def kernel(
    amp, chol_t, chol, out,
    rows_l, win, amps, ints, total, turned, parts,
    loc_sem, t_sem, w_sem, p_sem, l_sem, r_sem, s_sem,
):
    g, p = lax.axis_index("grp"), lax.axis_index("pair")
    x, y_lo, h = p // 4, (p // 2) % 2, p % 2
    y_hi, z = g // 4, g % 4
    y = 2 * y_hi + y_lo
    xr, xl = (x + 1) % 4, (x + 3) % 4
    zu, zd, zf = (z + 1) % 4, (z + 3) % 4, (z + 2) % 4
    y_l = 2 * y_hi + (1 - y_lo)
    y_h = 2 * (1 - y_hi) + (1 - y_lo)
    y_f = 2 * (1 - y_hi) + y_lo

    def dev(xx, yy, zz, hh):
        return ((yy // 2) * 4 + zz, xx * 4 + (yy % 2) * 2 + hh)

    sib = dev(x, y, z, 1 - h)
    right, left = dev(xr, y, z, h), dev(xl, y, z, h)
    lo, hi = dev(x, y_l, z, h), dev(x, y_h, z, h)
    up, down = dev(x, y, zu, h), dev(x, y, zd, h)

    started = []
    n_sent = [0]

    def remote(src, dst, recv, to, k):
        return pltpu.make_async_remote_copy(
            src_ref=src, dst_ref=dst, send_sem=s_sem.at[k], recv_sem=recv, device_id=to, device_id_type=MESH
        )

    def send(src, dst, recv, to):
        c = remote(src, dst, recv, to, n_sent[0])
        n_sent[0] += 1
        c.start()
        started.append(c)

    def arrived(dst, recv):
        remote(dst, dst, recv, sib, 0).wait_recv()

    def blk(i):
        return amps.at[i]

    def wblk(a, zz):
        return win.at[zz // 2, a, zz % 2]

    def piece(a, zz, j):
        return win.at[zz // 2, a, zz % 2, pl.ds(16 * j, 16)]

    def send_t(i, to):
        send(blk(i), blk(i), t_sem.at[i], to)

    def send_w(a, zz, to):
        send(wblk(a, zz), wblk(a, zz), w_sem.at[a * 4 + zz], to)

    def wait_t(i):
        arrived(blk(i), t_sem.at[i])

    def wait_w(a, zz):
        arrived(wblk(a, zz), w_sem.at[a * 4 + zz])

    half = pl.ds(pl.multiple_of(h * 256, 256), 256)
    other = pl.ds(pl.multiple_of((1 - h) * 256, 256), 256)
    own_t = pltpu.make_async_copy(amp.at[:, :, half], blk(p), loc_sem.at[0])
    own_t.start()
    own_l = pltpu.make_async_copy(chol_t, rows_l.at[h], loc_sem.at[1])
    own_l.start()

    barrier = pltpu.get_barrier_semaphore()

    def hello(to):
        pl.semaphore_signal(barrier, inc=1, device_id=to, device_id_type=MESH)

    me = g * 2 + h

    def peer(o):
        i = (me + o) % 16
        return i // 2, (p // 2) * 2 + i % 2, i

    for to in (right, left, lo, hi):
        hello(to)
    for o in range(1, 16):
        hello(peer(o)[:2])
    is_source = p == 0

    @pl.when((x != 2) & jnp.logical_not(is_source & (g < 4)))
    def _():
        hello((h * 4 + z, 0))

    @pl.when(jnp.logical_not(is_source))
    def _():
        pl.semaphore_wait(barrier, 19)

    @pl.when(is_source & (y_hi == 0))
    def _():
        pl.semaphore_wait(barrier, 30)

    @pl.when(is_source & (y_hi == 1))
    def _():
        pl.semaphore_wait(barrier, 31)

    n_scatter = n_sent[0]

    def scatter(top):
        k = n_scatter
        for qy in ((2 * top + 2) % 4, (2 * top + 1) % 4, (2 * top + 3) % 4, 2 * top):
            for j in (1, 3, 0, 2):
                src, dst = chol.at[qy, pl.ds(16 * j, 16)], piece(qy, z, j)
                if top == 0 and qy == 0 and X_OF_PIECE[j] == 0:
                    yield None, pltpu.make_async_copy(src, dst, p_sem.at[j])
                else:
                    yield remote(src, dst, p_sem.at[j], dev(X_OF_PIECE[j], qy, z, top), k), None
                    k += 1

    for top in (0, 1):

        @pl.when(is_source & (y_hi == top))
        def _():
            for away, here in scatter(top):
                (away or here).start()

    n_sent[0] = n_scatter + 16

    send(amp.at[:, :, other], blk(p), t_sem.at[p], sib)
    own_t.wait()
    for to in (right, left, lo):
        send_t(p, to)
    send(chol_t, rows_l.at[h], l_sem, sib)

    n_row = n_sent[0]

    def got(j):
        arrived(piece(y, z, j), p_sem.at[j])

    def row(xx):
        k = n_row
        for j, tos in ROW_PLAN[xx]:
            copies = []
            for to in tos:
                copies.append(remote(piece(y, z, j), piece(y, z, j), p_sem.at[j], (left, right)[to], k))
                k += 1
            yield j, copies

    for xx in range(4):

        @pl.when(x == xx)
        def _():
            for j, copies in row(xx):
                got(j)
                for c in copies:
                    c.start()

    n_sent[0] = n_row + 6

    for to in (down, up, hi, lo):
        send_w(y, z, to)
    sib_p = (p // 2) * 2 + (1 - h)
    wait_t(sib_p)
    for to in (right, left, lo):
        send_t(sib_p, to)
    wait_w(y_l, z)
    for to in (down, up, hi):
        send_w(y_l, z, to)
    lo_p = x * 4 + (1 - y_lo) * 2 + h
    lo_s = x * 4 + (1 - y_lo) * 2 + (1 - h)
    wait_t(lo_p)
    for to in (right, left):
        send_t(lo_p, to)
    wait_w(y, zd)
    send_w(y, zd, hi)
    wait_w(y, zu)
    send_w(y, zu, hi)
    send_w(y, zu, down)
    wait_w(y_f, z)
    for to in (down, up):
        send_w(y_f, z, to)
    fr = xl * 4 + y_lo * 2
    fl = xr * 4 + (1 - y_lo) * 2
    wait_t(fr + h)
    send_t(fr + h, right)
    wait_t(lo_s)
    for to in (right, left):
        send_t(lo_s, to)
    wait_t(fl + h)
    send_t(fl + h, left)
    wait_t(fr + (1 - h))
    send_t(fr + (1 - h), right)

    wait_w(y_l, zd)
    send_w(y_l, zd, up)
    wait_w(y_l, zu)

    own_l.wait()
    arrived(rows_l.at[1 - h], l_sem)

    wide = ROW_CHUNK // 32

    def tile(zz, aa):
        w = win[zz, pl.ds(2 * aa, 2)].reshape(256, 2048)
        lanes = pl.ds(pl.multiple_of(zz * 128, 128), 128)

        def body(i, carry):
            k, d0 = i // (64 // wide), (i % (64 // wide)) * wide
            l = rows_l[k, pl.ds(d0, wide)].reshape(ROW_CHUNK, 2048)
            o = lax.dot_general(l, w, (((1,), (1,)), ((), ())), preferred_element_type=F32).astype(BF16)
            for q in (0, 1):
                ints[pl.ds(d0, wide), k * 4 + 2 * aa + q, :, lanes] = o[:, q * 128 : q * 128 + 128].reshape(
                    wide, 32, 128
                )
            return carry

        lax.fori_loop(0, 2 * (64 // wide), body, 0)

    zz, aa = z // 2, y // 2
    tile(zz, aa)

    wait_t(fl + (1 - h))
    send_t(fl + (1 - h), left)
    wait_w(y_h, zd)
    send_w(y_h, zd, up)
    wait_w(y_f, zu)
    send_w(y_f, zu, down)
    wait_w(y_h, zu)
    wait_w(y_h, z)
    wait_w(y_f, zd)
    tile(zz, 1 - aa)
    wait_w(y, zf)
    wait_w(y_l, zf)
    tile(1 - zz, aa)
    wait_w(y_f, zf)
    wait_w(y_h, zf)
    tile(1 - zz, 1 - aa)

    for k in (0, 1):
        wait_t(xr * 4 + y_lo * 2 + k)
        wait_t(xl * 4 + (1 - y_lo) * 2 + k)
    for k in range(4):
        wait_t(((x + 2) % 4) * 4 + k)

    total[...] = jnp.zeros_like(total)

    def step(i, carry):
        acc = None
        for u in range(4):
            d = i * 4 + u
            o = lax.dot_general(
                ints[d].reshape(256, 256), amps[:, d].reshape(128, 256), (((1,), (1,)), ((), ())),
                preferred_element_type=F32,
            )
            acc = o if acc is None else acc + o
        total[...] += acc
        return carry

    lax.fori_loop(0, 16, step, 0)
    turned[...] = total[...].T

    for o in range(1, 16):
        gg, pp, i = peer(o)
        send(
            turned.at[pl.ds(pl.multiple_of(gg * 16, 16), 16), pl.ds(pl.multiple_of((i % 2) * 128, 128), 128)],
            parts.at[me], r_sem.at[me], (gg, pp),
        )
    acc = turned[pl.ds(pl.multiple_of(g * 16, 16), 16), pl.ds(pl.multiple_of(h * 128, 128), 128)]
    for o in range(1, 16):
        i = peer(o)[2]
        arrived(parts.at[i], r_sem.at[i])
        acc = acc + parts[i]
    for a in range(A_WIN):
        out[a] = acc[:, a * 32 : a * 32 + 32]

    for c in started:
        c.wait_send()
    for top in (0, 1):

        @pl.when(is_source & (y_hi == top))
        def _():
            for away, _ in scatter(top):
                if away is not None:
                    away.wait_send()

    for xx in (0, 1, 3):

        @pl.when(x == xx)
        def _():
            for _, copies in row(xx):
                for c in copies:
                    c.wait_send()


def per_device(amplitudes, cholesky):
    hbm = pl.BlockSpec(memory_space=pltpu.MemorySpace.HBM)
    out = pl.pallas_call(
        kernel,
        out_shape=jax.ShapeDtypeStruct((A_WIN, 16, 32), F32),
        in_specs=[hbm] * 3,
        out_specs=pl.BlockSpec(memory_space=pltpu.VMEM),
        scratch_shapes=[
            pltpu.VMEM((2, 64, 32, 2048), BF16),
            pltpu.VMEM((2, A_WIN, 2, 64, 2048), BF16),
            pltpu.VMEM((16, 64, 8, 256), BF16),
            pltpu.VMEM((64, 8, 32, 256), BF16),
            pltpu.VMEM((256, 128), F32),
            pltpu.VMEM((128, 256), F32),
            pltpu.VMEM((16, 16, 128), F32),
            pltpu.SemaphoreType.DMA((2,)),
            pltpu.SemaphoreType.DMA((16,)),
            pltpu.SemaphoreType.DMA((16,)),
            pltpu.SemaphoreType.DMA((4,)),
            pltpu.SemaphoreType.DMA,
            pltpu.SemaphoreType.DMA((16,)),
            pltpu.SemaphoreType.DMA((80,)),
        ],
        compiler_params=pltpu.CompilerParams(
            collective_id=0, has_side_effects=True, vmem_limit_bytes=56 * 2**20
        ),
    )(amplitudes.transpose(1, 0, 2), cholesky.transpose(1, 0, 2), cholesky)
    return out.transpose(2, 0, 1)


def solution(mesh):
    in_specs = (P("pair", "grp", None), P("pair", "grp", None))
    out_specs = P("pair", None, "grp")
    return jax.shard_map(
        per_device, mesh=mesh, in_specs=in_specs, out_specs=out_specs, check_vma=False
    )
```

```python
import jax
import jax.numpy as jnp
from jax import lax
from jax.experimental import pallas as pl
from jax.experimental.pallas import tpu as pltpu
from jax.sharding import PartitionSpec as P

A_WIN = 4
MESH = pl.DeviceIdType.MESH
F32, BF16 = jnp.float32, jnp.bfloat16


ROW_CHUNK = 1024
X_OF_PIECE = (0, 1, 0, 3)
ROW_PLAN = (
    (((0, (1, 0)), (2, (1, 0))), ((1, (0,)), (3, (1,)))),
    (((1, (0, 1)),), ((0, (1,)), (2, ()), (3, ()))),
    ((), ((1, ()), (3, ()), (0, ()), (2, ()))),
    (((3, (1, 0)),), ((2, (0,)), (0, ()), (1, ()))),
)


def kernel(
    amp, chol, out,
    raw_l, raw_t, out_t, rows_l, win, amps, ints, total, turned, parts,
    loc_sem, t_sem, w_sem, p_sem, l_sem, r_sem, s_sem,
):
    g, p = lax.axis_index("grp"), lax.axis_index("pair")
    x, y_lo, h = p // 4, (p // 2) % 2, p % 2
    y_hi, z = g // 4, g % 4
    y = 2 * y_hi + y_lo
    xr, xl = (x + 1) % 4, (x + 3) % 4
    zu, zd, zf = (z + 1) % 4, (z + 3) % 4, (z + 2) % 4
    y_l = 2 * y_hi + (1 - y_lo)
    y_h = 2 * (1 - y_hi) + (1 - y_lo)
    y_f = 2 * (1 - y_hi) + y_lo

    def dev(xx, yy, zz, hh):
        return ((yy // 2) * 4 + zz, xx * 4 + (yy % 2) * 2 + hh)

    sib = dev(x, y, z, 1 - h)
    right, left = dev(xr, y, z, h), dev(xl, y, z, h)
    lo, hi = dev(x, y_l, z, h), dev(x, y_h, z, h)
    up, down = dev(x, y, zu, h), dev(x, y, zd, h)

    started = []
    n_sent = [0]

    def remote(src, dst, recv, to, k):
        return pltpu.make_async_remote_copy(
            src_ref=src, dst_ref=dst, send_sem=s_sem.at[k], recv_sem=recv, device_id=to, device_id_type=MESH
        )

    def send(src, dst, recv, to):
        c = remote(src, dst, recv, to, n_sent[0])
        n_sent[0] += 1
        c.start()
        started.append(c)

    def arrived(dst, recv):
        remote(dst, dst, recv, sib, 0).wait_recv()

    def blk(i):
        return amps.at[i]

    def wblk(a, zz):
        return win.at[zz // 2, a, zz % 2]

    def piece(a, zz, j):
        return win.at[zz // 2, a, zz % 2, pl.ds(16 * j, 16)]

    def send_t(i, to):
        send(blk(i), blk(i), t_sem.at[i], to)

    def send_w(a, zz, to):
        send(wblk(a, zz), wblk(a, zz), w_sem.at[a * 4 + zz], to)

    def wait_t(i):
        arrived(blk(i), t_sem.at[i])

    def wait_w(a, zz):
        arrived(wblk(a, zz), w_sem.at[a * 4 + zz])

    half = pl.ds(pl.multiple_of(h * 256, 256), 256)
    other = pl.ds(pl.multiple_of((1 - h) * 256, 256), 256)

    def turn(i):
        own_l[i].wait()

        def body(n, carry):
            lanes = pl.ds(pl.multiple_of(n * 256, 256), 256)
            rows_l[h, pl.ds(16 * i, 16), :, lanes] = jnp.swapaxes(raw_l[:, pl.ds(16 * i, 16), lanes], 0, 1)
            return carry

        lax.fori_loop(0, 8, body, 0)

    own_t = pltpu.make_async_copy(amp, raw_t, loc_sem.at[4])
    own_t.start()
    own_l = [
        pltpu.make_async_copy(chol.at[:, pl.ds(16 * i, 16)], raw_l.at[:, pl.ds(16 * i, 16)], loc_sem.at[i])
        for i in range(4)
    ]
    for c in own_l:
        c.start()

    barrier = pltpu.get_barrier_semaphore()

    def hello(to):
        pl.semaphore_signal(barrier, inc=1, device_id=to, device_id_type=MESH)

    me = g * 2 + h

    def peer(o):
        i = (me + o) % 16
        return i // 2, (p // 2) * 2 + i % 2, i

    for to in (sib, right, left, lo, hi, up, down):
        hello(to)
    is_source = p == 0

    @pl.when((x != 2) & jnp.logical_not(is_source & (g < 4)))
    def _():
        hello((h * 4 + z, 0))

    own_t.wait()
    amps[p] = jnp.swapaxes(raw_t[:, :, half], 0, 1)
    out_t[...] = jnp.swapaxes(raw_t[:, :, other], 0, 1)
    turn(0)
    turn(1)

    @pl.when(jnp.logical_not(is_source))
    def _():
        pl.semaphore_wait(barrier, 7)

    @pl.when(is_source & (y_hi == 0))
    def _():
        pl.semaphore_wait(barrier, 18)

    @pl.when(is_source & (y_hi == 1))
    def _():
        pl.semaphore_wait(barrier, 19)

    n_scatter = n_sent[0]

    def scatter(top):
        k = n_scatter
        for qy in ((2 * top + 2) % 4, (2 * top + 1) % 4, (2 * top + 3) % 4, 2 * top):
            for j in (1, 3, 0, 2):
                src, dst = chol.at[qy, pl.ds(16 * j, 16)], piece(qy, z, j)
                if top == 0 and qy == 0 and X_OF_PIECE[j] == 0:
                    yield None, pltpu.make_async_copy(src, dst, p_sem.at[j])
                else:
                    yield remote(src, dst, p_sem.at[j], dev(X_OF_PIECE[j], qy, z, top), k), None
                    k += 1

    for top in (0, 1):

        @pl.when(is_source & (y_hi == top))
        def _():
            for away, here in scatter(top):
                (away or here).start()

    n_sent[0] = n_scatter + 16

    send(out_t, blk(p), t_sem.at[p], sib)

    def send_t_part(d, n, to):
        send(blk(p).at[pl.ds(d, n)], blk(p).at[pl.ds(d, n)], t_sem.at[p], to)

    send_t_part(0, 16, right)
    send_t_part(0, 16, left)
    send_t(p, lo)
    turn(2)
    turn(3)
    send(rows_l.at[h], rows_l.at[h], l_sem, sib)

    def got(j):
        arrived(piece(y, z, j), p_sem.at[j])

    def row(xx, part, k):
        for j, tos in ROW_PLAN[xx][part]:
            quarter = piece(y, z, j)
            copies = []
            for recv, to in [(p_sem.at[j], (left, right)[t]) for t in tos] + [
                (w_sem.at[y * 4 + z], to) for to in (down, up, hi, lo)
            ]:
                copies.append(remote(quarter, quarter, recv, to, k))
                k += 1
            yield j, copies

    n_row = []
    for part in (0, 1):
        n_row.append(n_sent[0])
        for xx in range(4):
            if ROW_PLAN[xx][part]:

                @pl.when(x == xx)
                def _():
                    for j, copies in row(xx, part, n_row[part]):
                        got(j)
                        for c in copies:
                            c.start()

        n_sent[0] += 18
        if part == 0:
            send_t_part(16, 16, right)
            send_t_part(16, 16, left)
    send_t_part(32, 32, right)
    send_t_part(32, 32, left)

    mine = x * 4 + y_lo * 2
    sib_p = mine + (1 - h)
    lo_p = x * 4 + (1 - y_lo) * 2 + h
    lo_s = x * 4 + (1 - y_lo) * 2 + (1 - h)
    fr = xl * 4 + y_lo * 2
    gr = xr * 4 + y_lo * 2
    fl = xr * 4 + (1 - y_lo) * 2
    gl = xl * 4 + (1 - y_lo) * 2
    wait_t(sib_p)
    for to in (right, left, lo):
        send_t(sib_p, to)
    wait_w(y_l, z)
    for to in (down, up, hi):
        send_w(y_l, z, to)
    wait_t(lo_p)
    for to in (right, left):
        send_t(lo_p, to)
    wait_w(y, zd)
    send_w(y, zd, hi)
    wait_w(y, zu)
    send_w(y, zu, hi)
    send_w(y, zu, down)
    wait_t(fr + h)
    send_t(fr + h, right)
    wait_w(y_l, zd)
    send_w(y_l, zd, up)
    wait_w(y_l, zu)

    arrived(rows_l.at[1 - h], l_sem)

    wide = ROW_CHUNK // 32

    def tile(zz, aa):
        w = win[zz, pl.ds(2 * aa, 2)].reshape(256, 2048)
        lanes = pl.ds(pl.multiple_of(zz * 128, 128), 128)

        def body(i, carry):
            k, d0 = i // (64 // wide), (i % (64 // wide)) * wide
            l = rows_l[k, pl.ds(d0, wide)].reshape(ROW_CHUNK, 2048)
            o = lax.dot_general(l, w, (((1,), (1,)), ((), ())), preferred_element_type=F32).astype(BF16)
            for q in (0, 1):
                ints[pl.ds(d0, wide), k * 4 + 2 * aa + q, :, lanes] = o[:, q * 128 : q * 128 + 128].reshape(
                    wide, 32, 128
                )
            return carry

        lax.fori_loop(0, 2 * (64 // wide), body, 0, unroll=True)

    zz, aa = z // 2, y // 2
    tile(zz, aa)

    wait_w(y_f, z)
    for to in (down, up):
        send_w(y_f, z, to)
    wait_t(fr + (1 - h))
    send_t(fr + (1 - h), lo)
    send_t(fr + (1 - h), right)
    wait_t(gr + (1 - h))
    send_t(gr + (1 - h), lo)
    wait_t(fl + h)
    send_t(fl + h, left)
    wait_w(y_h, zd)
    send_w(y_h, zd, up)
    wait_w(y, zf)
    wait_w(y_l, zf)
    tile(1 - zz, aa)

    wait_w(y_f, zu)
    send_w(y_f, zu, down)
    wait_t(fl + (1 - h))
    send_t(fl + (1 - h), left)
    wait_w(y_h, zu)
    wait_w(y_h, z)
    wait_w(y_f, zd)
    tile(zz, 1 - aa)
    wait_w(y_f, zf)
    wait_w(y_h, zf)
    tile(1 - zz, 1 - aa)

    wait_t(lo_s)
    wait_t(gr + h)
    for k in (0, 1):
        wait_t(gl + k)
    for k in range(4):
        wait_t(((x + 2) % 4) * 4 + k)

    total[...] = jnp.zeros_like(total)

    def step(i, carry):
        acc = None
        for u in range(16):
            d = i * 16 + u
            o = lax.dot_general(
                ints[d].reshape(256, 256), amps[:, d].reshape(128, 256), (((1,), (1,)), ((), ())),
                preferred_element_type=F32,
            )
            acc = o if acc is None else acc + o
        total[...] += acc
        return carry

    lax.fori_loop(0, 4, step, 0)
    turned[...] = total[...].T

    for c in started:
        c.wait_send()
    started.clear()
    for top in (0, 1):

        @pl.when(is_source & (y_hi == top))
        def _():
            for away, _ in scatter(top):
                if away is not None:
                    away.wait_send()

    for part in (0, 1):
        for xx in range(4):
            if ROW_PLAN[xx][part]:

                @pl.when(x == xx)
                def _():
                    for _, copies in row(xx, part, n_row[part]):
                        for c in copies:
                            c.wait_send()

    for o in range(1, 16):
        gg, pp, i = peer(o)
        send(
            turned.at[pl.ds(pl.multiple_of(gg * 16, 16), 16), pl.ds(pl.multiple_of((i % 2) * 128, 128), 128)],
            parts.at[me], r_sem.at[me], (gg, pp),
        )
    acc = turned[pl.ds(pl.multiple_of(g * 16, 16), 16), pl.ds(pl.multiple_of(h * 128, 128), 128)]
    for o in range(1, 16):
        i = peer(o)[2]
        arrived(parts.at[i], r_sem.at[i])
        acc = acc + parts[i]
    for a in range(A_WIN):
        out[a] = acc[:, a * 32 : a * 32 + 32]

    for c in started:
        c.wait_send()


def per_device(amplitudes, cholesky):
    hbm = pl.BlockSpec(memory_space=pltpu.MemorySpace.HBM)
    out = pl.pallas_call(
        kernel,
        out_shape=jax.ShapeDtypeStruct((A_WIN, 16, 32), F32),
        in_specs=[hbm] * 2,
        out_specs=pl.BlockSpec(memory_space=pltpu.VMEM),
        scratch_shapes=[
            pltpu.VMEM((32, 64, 2048), BF16),
            pltpu.VMEM((8, 64, 512), BF16),
            pltpu.VMEM((64, 8, 256), BF16),
            pltpu.VMEM((2, 64, 32, 2048), BF16),
            pltpu.VMEM((2, A_WIN, 2, 64, 2048), BF16),
            pltpu.VMEM((16, 64, 8, 256), BF16),
            pltpu.VMEM((64, 8, 32, 256), BF16),
            pltpu.VMEM((256, 128), F32),
            pltpu.VMEM((128, 256), F32),
            pltpu.VMEM((16, 16, 128), F32),
            pltpu.SemaphoreType.DMA((5,)),
            pltpu.SemaphoreType.DMA((16,)),
            pltpu.SemaphoreType.DMA((16,)),
            pltpu.SemaphoreType.DMA((4,)),
            pltpu.SemaphoreType.DMA,
            pltpu.SemaphoreType.DMA((16,)),
            pltpu.SemaphoreType.DMA((112,)),
        ],
        compiler_params=pltpu.CompilerParams(
            collective_id=0, has_side_effects=True, vmem_limit_bytes=56 * 2**20
        ),
    )(amplitudes, cholesky)
    return out.transpose(2, 0, 1)


def solution(mesh):
    in_specs = (P("pair", "grp", None), P("pair", "grp", None))
    out_specs = P("pair", None, "grp")
    return jax.shard_map(
        per_device, mesh=mesh, in_specs=in_specs, out_specs=out_specs, check_vma=False
    )
```

```python
import jax
import jax.numpy as jnp
from jax import lax
from jax.experimental import pallas as pl
from jax.experimental.pallas import tpu as pltpu
from jax.sharding import PartitionSpec as P

A_WIN = 4
MESH = pl.DeviceIdType.MESH
F32, BF16 = jnp.float32, jnp.bfloat16


ROW_CHUNK = 1024
ENTRIES = (((0, 0), (0, 2), (1, 1), (3, 3)), ((0, 1), (0, 3)))
ROW_PLAN = (
    ((0, (1, 0)), (2, (1, 0)), (1, (0,)), (3, (1,))),
    ((1, (1,)), (0, (1,)), (2, ()), (3, ())),
    ((1, ()), (3, ()), (0, ()), (2, ())),
    ((3, (0,)), (2, (0,)), (0, ()), (1, ())),
)


def kernel(
    amp, chol, out,
    raw_l, raw_t, out_t, rows_l, win, amps, ints, total, turned, parts,
    loc_sem, t_sem, w_sem, p_sem, q_sem, u_sem, v_sem, l_sem, r_sem, s_sem,
):
    g, p = lax.axis_index("grp"), lax.axis_index("pair")
    x, y_lo, h = p // 4, (p // 2) % 2, p % 2
    y_hi, z = g // 4, g % 4
    y = 2 * y_hi + y_lo
    xr, xl = (x + 1) % 4, (x + 3) % 4
    zu, zd, zf = (z + 1) % 4, (z + 3) % 4, (z + 2) % 4
    y_l = 2 * y_hi + (1 - y_lo)
    y_h = 2 * (1 - y_hi) + (1 - y_lo)
    y_f = 2 * (1 - y_hi) + y_lo

    def dev(xx, yy, zz, hh):
        return ((yy // 2) * 4 + zz, xx * 4 + (yy % 2) * 2 + hh)

    sib = dev(x, y, z, 1 - h)
    right, left = dev(xr, y, z, h), dev(xl, y, z, h)
    lo, hi = dev(x, y_l, z, h), dev(x, y_h, z, h)
    up, down = dev(x, y, zu, h), dev(x, y, zd, h)

    started = []
    n_sent = [0]

    def remote(src, dst, recv, to, k):
        return pltpu.make_async_remote_copy(
            src_ref=src, dst_ref=dst, send_sem=s_sem.at[k], recv_sem=recv, device_id=to, device_id_type=MESH
        )

    def send(src, dst, recv, to):
        c = remote(src, dst, recv, to, n_sent[0])
        n_sent[0] += 1
        c.start()
        started.append(c)

    def arrived(dst, recv):
        remote(dst, dst, recv, sib, 0).wait_recv()

    def blk(i):
        return amps.at[i]

    def wblk(a, zz):
        return win.at[zz // 2, a, zz % 2]

    def piece(a, zz, j):
        return win.at[zz // 2, a, zz % 2, pl.ds(16 * j, 16)]

    def send_t(i, to):
        send(blk(i), blk(i), t_sem.at[i], to)

    def send_w(a, zz, to):
        send(wblk(a, zz), wblk(a, zz), w_sem.at[a * 4 + zz], to)

    def wait_t(i):
        arrived(blk(i), t_sem.at[i])

    def wait_w(a, zz):
        arrived(wblk(a, zz), w_sem.at[a * 4 + zz])

    half = pl.ds(pl.multiple_of(h * 256, 256), 256)
    other = pl.ds(pl.multiple_of((1 - h) * 256, 256), 256)

    def turn(i):
        own_l[i].wait()

        def body(n, carry):
            lanes = pl.ds(pl.multiple_of(n * 256, 256), 256)
            rows_l[h, pl.ds(16 * i, 16), :, lanes] = jnp.swapaxes(raw_l[:, pl.ds(16 * i, 16), lanes], 0, 1)
            return carry

        lax.fori_loop(0, 8, body, 0)

    own_t = pltpu.make_async_copy(amp, raw_t, loc_sem.at[4])
    own_t.start()
    own_l = [
        pltpu.make_async_copy(chol.at[:, pl.ds(16 * i, 16)], raw_l.at[:, pl.ds(16 * i, 16)], loc_sem.at[i])
        for i in range(4)
    ]
    for c in own_l:
        c.start()

    barrier = pltpu.get_barrier_semaphore()

    def hello(to):
        pl.semaphore_signal(barrier, inc=1, device_id=to, device_id_type=MESH)

    me = g * 2 + h

    def peer(o):
        i = (me + o) % 16
        return i // 2, (p // 2) * 2 + i % 2, i

    for to in (sib, right, left, lo, hi, up, down):
        hello(to)
    is_source = p == 0

    @pl.when((x != 2) & jnp.logical_not(is_source & (g < 4)))
    def _():
        hello((h * 4 + z, 0))

    own_t.wait()
    amps[p] = jnp.swapaxes(raw_t[:, :, half], 0, 1)
    out_t[...] = jnp.swapaxes(raw_t[:, :, other], 0, 1)
    turn(0)
    turn(1)

    @pl.when(jnp.logical_not(is_source))
    def _():
        pl.semaphore_wait(barrier, 7)

    @pl.when(is_source & (y_hi == 0))
    def _():
        pl.semaphore_wait(barrier, 18)

    @pl.when(is_source & (y_hi == 1))
    def _():
        pl.semaphore_wait(barrier, 19)

    n_scatter = n_sent[0]

    def scatter(top):
        k = n_scatter
        for entries in ENTRIES:
            for qy in ((2 * top + 2) % 4, (2 * top + 1) % 4, (2 * top + 3) % 4, 2 * top):
                for to_x, j in entries:
                    src, dst = chol.at[qy, pl.ds(16 * j, 16)], piece(qy, z, j)
                    if top == 0 and qy == 0 and to_x == 0:
                        yield None, pltpu.make_async_copy(src, dst, p_sem.at[j])
                    else:
                        yield remote(src, dst, p_sem.at[j], dev(to_x, qy, z, top), k), None
                        k += 1

    for top in (0, 1):

        @pl.when(is_source & (y_hi == top))
        def _():
            for away, here in scatter(top):
                (away or here).start()

    n_sent[0] = n_scatter + 24

    send(out_t, blk(p), t_sem.at[p], sib)

    def send_t_part(d, n, to):
        send(blk(p).at[pl.ds(d, n)], blk(p).at[pl.ds(d, n)], t_sem.at[p], to)

    send_t_part(0, 16, right)
    send_t_part(0, 16, left)
    turn(2)
    turn(3)
    send(rows_l.at[h], rows_l.at[h], l_sem, sib)

    def got(j):
        arrived(piece(y, z, j), p_sem.at[j])

    def row(xx, k):
        for j, tos in ROW_PLAN[xx]:
            quarter = piece(y, z, j)
            copies = []
            for recv, to in [(p_sem.at[j], (left, right)[t]) for t in tos] + [
                (w_sem.at[y * 4 + z], down), (w_sem.at[y * 4 + z], up), (q_sem.at[j], lo), (w_sem.at[y * 4 + z], hi)
            ]:
                copies.append(remote(quarter, quarter, recv, to, k))
                k += 1
            yield j, copies

    def row_l(xx, k):
        for j, _ in ROW_PLAN[xx]:
            quarter = piece(y_l, z, j)
            block = w_sem.at[y_l * 4 + z]
            yield j, [
                remote(quarter, quarter, recv, to, k + n)
                for n, (recv, to) in enumerate(((block, down), (u_sem.at[j], up), (block, hi)))
            ]
            k += 3

    def row_u(xx, k):
        for j, _ in ROW_PLAN[xx]:
            quarter = piece(y_l, zd, j)
            yield j, [remote(quarter, quarter, w_sem.at[y_l * 4 + zd], up, k)]
            k += 1

    n_row = n_sent[0]
    for xx in range(4):

        @pl.when(x == xx)
        def _():
            for j, copies in row(xx, n_row):
                got(j)
                for c in copies:
                    c.start()

    n_sent[0] += 22
    mine = x * 4 + y_lo * 2
    sib_p = mine + (1 - h)
    lo_p = x * 4 + (1 - y_lo) * 2 + h
    lo_s = x * 4 + (1 - y_lo) * 2 + (1 - h)
    fr = xl * 4 + y_lo * 2
    gr = xr * 4 + y_lo * 2
    fl = xr * 4 + (1 - y_lo) * 2
    gl = xl * 4 + (1 - y_lo) * 2
    wait_t(sib_p)
    for to in (right, left):
        send_t(sib_p, to)
    for to in (right, left):
        send_t_part(16, 48, to)
    send_t(p, lo)
    send_t(sib_p, lo)
    n_row_l = n_sent[0]
    for xx in range(4):

        @pl.when(x == xx)
        def _():
            for j, copies in row_l(xx, n_row_l):
                arrived(piece(y_l, z, j), q_sem.at[j])
                for c in copies:
                    c.start()

    n_sent[0] += 12
    wait_w(y, zd)
    send_w(y, zd, hi)
    wait_w(y, zu)
    send_w(y, zu, hi)
    send_w(y, zu, down)
    n_row_u = n_sent[0]
    for xx in range(4):

        @pl.when(x == xx)
        def _():
            for j, copies in row_u(xx, n_row_u):
                arrived(piece(y_l, zd, j), u_sem.at[j])
                for c in copies:
                    c.start()

    n_sent[0] += 4
    wait_w(y_l, zu)
    arrived(rows_l.at[1 - h], l_sem)

    wide = ROW_CHUNK // 32

    def tile(zz, aa, halves=(0, 1)):
        w = win[zz, pl.ds(2 * aa, 2)].reshape(256, 2048)
        lanes = pl.ds(pl.multiple_of(zz * 128, 128), 128)
        for k in halves:
            for d0 in range(0, 64, wide):
                l = rows_l[k, pl.ds(d0, wide)].reshape(ROW_CHUNK, 2048)
                o = lax.dot_general(l, w, (((1,), (1,)), ((), ())), preferred_element_type=F32).astype(BF16)
                for q in (0, 1):
                    ints[pl.ds(d0, wide), k * 4 + 2 * aa + q, :, lanes] = o[:, q * 128 : q * 128 + 128].reshape(
                        wide, 32, 128
                    )

    zz, aa = z // 2, y // 2
    tile(zz, aa, (0,))
    wait_w(y_f, z)
    for q in (0, 1):
        half_w = wblk(y_f, z).at[pl.ds(32 * q, 32)]
        send(half_w, half_w, v_sem.at[q], down)
    send_w(y_f, z, up)
    wait_t(fr + (1 - h))
    send_t(fr + (1 - h), lo)
    send_t(fr + (1 - h), right)
    wait_t(gr + (1 - h))
    send_t(gr + (1 - h), lo)
    wait_t(lo_p)
    for to in (right, left):
        send_t(lo_p, to)
    tile(zz, aa, (1,))

    wait_t(fr + h)
    send_t(fr + h, right)
    wait_w(y, zf)
    send_w(y, zf, hi)
    wait_w(y_l, zf)

    def forward_f(q):
        half_w = wblk(y_f, zu).at[pl.ds(32 * q, 32)]
        arrived(half_w, v_sem.at[q])
        send(half_w, half_w, w_sem.at[y_f * 4 + zu], down)

    tile(1 - zz, aa, (0,))
    forward_f(0)
    tile(1 - zz, aa, (1,))
    forward_f(1)
    wait_t(fl + h)
    send_t(fl + h, left)
    away = ((x + 2) % 4) * 4
    wait_t(away + y_lo * 2 + (1 - h))
    send_t(away + y_lo * 2 + (1 - h), lo)

    wait_w(y_h, zu)
    wait_w(y_h, zd)
    wait_w(y_h, z)
    wait_w(y_f, zd)
    tile(zz, 1 - aa)
    wait_w(y_f, zf)
    wait_w(y_h, zf)
    tile(1 - zz, 1 - aa)

    wait_t(lo_s)
    wait_t(gr + h)
    for k in (0, 1):
        wait_t(gl + k)
    wait_t(fl + (1 - h))
    wait_t(away + y_lo * 2 + h)
    for k in (0, 1):
        wait_t(away + (1 - y_lo) * 2 + k)

    total[...] = jnp.zeros_like(total)

    def step(i, carry):
        acc = None
        for u in range(16):
            d = i * 16 + u
            o = lax.dot_general(
                ints[d].reshape(256, 256), amps[:, d].reshape(128, 256), (((1,), (1,)), ((), ())),
                preferred_element_type=F32,
            )
            acc = o if acc is None else acc + o
        total[...] += acc
        return carry

    lax.fori_loop(0, 4, step, 0)
    turned[...] = total[...].T

    for c in started:
        c.wait_send()
    started.clear()
    for top in (0, 1):

        @pl.when(is_source & (y_hi == top))
        def _():
            for away, _ in scatter(top):
                if away is not None:
                    away.wait_send()

    for xx in range(4):

        @pl.when(x == xx)
        def _():
            for _, copies in (*row(xx, n_row), *row_l(xx, n_row_l), *row_u(xx, n_row_u)):
                for c in copies:
                    c.wait_send()

    for o in range(1, 16):
        gg, pp, i = peer(o)
        send(
            turned.at[pl.ds(pl.multiple_of(gg * 16, 16), 16), pl.ds(pl.multiple_of((i % 2) * 128, 128), 128)],
            parts.at[me], r_sem.at[me], (gg, pp),
        )
    acc = turned[pl.ds(pl.multiple_of(g * 16, 16), 16), pl.ds(pl.multiple_of(h * 128, 128), 128)]
    for o in range(1, 16):
        i = peer(o)[2]
        arrived(parts.at[i], r_sem.at[i])
        acc = acc + parts[i]
    for a in range(A_WIN):
        out[a] = acc[:, a * 32 : a * 32 + 32]

    for c in started:
        c.wait_send()


def per_device(amplitudes, cholesky):
    hbm = pl.BlockSpec(memory_space=pltpu.MemorySpace.HBM)
    out = pl.pallas_call(
        kernel,
        out_shape=jax.ShapeDtypeStruct((A_WIN, 16, 32), F32),
        in_specs=[hbm] * 2,
        out_specs=pl.BlockSpec(memory_space=pltpu.VMEM),
        scratch_shapes=[
            pltpu.VMEM((32, 64, 2048), BF16),
            pltpu.VMEM((8, 64, 512), BF16),
            pltpu.VMEM((64, 8, 256), BF16),
            pltpu.VMEM((2, 64, 32, 2048), BF16),
            pltpu.VMEM((2, A_WIN, 2, 64, 2048), BF16),
            pltpu.VMEM((16, 64, 8, 256), BF16),
            pltpu.VMEM((64, 8, 32, 256), BF16),
            pltpu.VMEM((256, 128), F32),
            pltpu.VMEM((128, 256), F32),
            pltpu.VMEM((16, 16, 128), F32),
            pltpu.SemaphoreType.DMA((5,)),
            pltpu.SemaphoreType.DMA((16,)),
            pltpu.SemaphoreType.DMA((16,)),
            pltpu.SemaphoreType.DMA((4,)),
            pltpu.SemaphoreType.DMA((4,)),
            pltpu.SemaphoreType.DMA((4,)),
            pltpu.SemaphoreType.DMA((2,)),
            pltpu.SemaphoreType.DMA,
            pltpu.SemaphoreType.DMA((16,)),
            pltpu.SemaphoreType.DMA((128,)),
        ],
        compiler_params=pltpu.CompilerParams(
            collective_id=0, has_side_effects=True, vmem_limit_bytes=56 * 2**20
        ),
    )(amplitudes, cholesky)
    return out.transpose(2, 0, 1)


def solution(mesh):
    in_specs = (P("pair", "grp", None), P("pair", "grp", None))
    out_specs = P("pair", None, "grp")
    return jax.shard_map(
        per_device, mesh=mesh, in_specs=in_specs, out_specs=out_specs, check_vma=False
    )
```

```python
import jax
import jax.numpy as jnp
from jax import lax
from jax.experimental import pallas as pl
from jax.experimental.pallas import tpu as pltpu
from jax.sharding import PartitionSpec as P

A_WIN = 4
MESH = pl.DeviceIdType.MESH
F32, BF16 = jnp.float32, jnp.bfloat16


ROW_CHUNK = 1024
PEERS = tuple((dy, dz, dk) for dy in (1, 0) for dz in (2, 1, 3, 0) for dk in (1, 0))[:15]
ENTRIES = (((0, 0), (0, 2), (1, 1), (3, 3)), ((0, 1), (0, 3)))
ROW_PLAN = (
    ((0, (1, 0)), (2, (1, 0)), (1, (0,)), (3, (1,))),
    ((1, (1,)), (0, (1,)), (2, ()), (3, ())),
    ((1, ()), (3, ()), (0, ()), (2, ())),
    ((3, (0,)), (2, (0,)), (0, ()), (1, ())),
)


def kernel(
    amp, chol, out,
    raw_l, raw_t, out_t, rows_l, win, amps, ints, total, turned, parts,
    loc_sem, t_sem, w_sem, p_sem, q_sem, u_sem, v_sem, l_sem, r_sem, s_sem,
):
    g, p = lax.axis_index("grp"), lax.axis_index("pair")
    x, y_lo, h = p // 4, (p // 2) % 2, p % 2
    y_hi, z = g // 4, g % 4
    y = 2 * y_hi + y_lo
    xr, xl = (x + 1) % 4, (x + 3) % 4
    zu, zd, zf = (z + 1) % 4, (z + 3) % 4, (z + 2) % 4
    y_l = 2 * y_hi + (1 - y_lo)
    y_h = 2 * (1 - y_hi) + (1 - y_lo)
    y_f = 2 * (1 - y_hi) + y_lo

    def dev(xx, yy, zz, hh):
        return ((yy // 2) * 4 + zz, xx * 4 + (yy % 2) * 2 + hh)

    sib = dev(x, y, z, 1 - h)
    right, left = dev(xr, y, z, h), dev(xl, y, z, h)
    lo, hi = dev(x, y_l, z, h), dev(x, y_h, z, h)
    up, down = dev(x, y, zu, h), dev(x, y, zd, h)

    started = []
    n_sent = [0]

    def remote(src, dst, recv, to, k):
        return pltpu.make_async_remote_copy(
            src_ref=src, dst_ref=dst, send_sem=s_sem.at[k], recv_sem=recv, device_id=to, device_id_type=MESH
        )

    def send(src, dst, recv, to):
        c = remote(src, dst, recv, to, n_sent[0])
        n_sent[0] += 1
        c.start()
        started.append(c)

    def arrived(dst, recv):
        remote(dst, dst, recv, sib, 0).wait_recv()

    def blk(i):
        return amps.at[i]

    def wblk(a, zz):
        return win.at[zz // 2, a, zz % 2]

    def piece(a, zz, j):
        return win.at[zz // 2, a, zz % 2, pl.ds(16 * j, 16)]

    def send_t(i, to):
        send(blk(i), blk(i), t_sem.at[i], to)

    def send_w(a, zz, to):
        send(wblk(a, zz), wblk(a, zz), w_sem.at[a * 4 + zz], to)

    def wait_t(i):
        arrived(blk(i), t_sem.at[i])

    def wait_w(a, zz):
        arrived(wblk(a, zz), w_sem.at[a * 4 + zz])

    half = pl.ds(pl.multiple_of(h * 256, 256), 256)
    other = pl.ds(pl.multiple_of((1 - h) * 256, 256), 256)

    def turn(i):
        own_l[i].wait()

        def body(n, carry):
            lanes = pl.ds(pl.multiple_of(n * 256, 256), 256)
            rows_l[h, pl.ds(16 * i, 16), :, lanes] = jnp.swapaxes(raw_l[:, pl.ds(16 * i, 16), lanes], 0, 1)
            return carry

        lax.fori_loop(0, 8, body, 0)

    own_t = pltpu.make_async_copy(amp, raw_t, loc_sem.at[4])
    own_t.start()
    own_l = [
        pltpu.make_async_copy(chol.at[:, pl.ds(16 * i, 16)], raw_l.at[:, pl.ds(16 * i, 16)], loc_sem.at[i])
        for i in range(4)
    ]
    for c in own_l:
        c.start()

    barrier = pltpu.get_barrier_semaphore()

    def hello(to):
        pl.semaphore_signal(barrier, inc=1, device_id=to, device_id_type=MESH)

    me = g * 2 + h

    def peer(o):
        dy, dz, dk = PEERS[o - 1]
        gg, k = ((y_hi + dy) % 2) * 4 + (z + dz) % 4, (h + dk) % 2
        return gg, (p // 2) * 2 + k, gg * 2 + k

    for to in (sib, right, left, lo, hi, up, down):
        hello(to)
    is_source = p == 0

    @pl.when((x != 2) & jnp.logical_not(is_source & (g < 4)))
    def _():
        hello((h * 4 + z, 0))

    own_t.wait()
    amps[p] = jnp.swapaxes(raw_t[:, :, half], 0, 1)
    out_t[...] = jnp.swapaxes(raw_t[:, :, other], 0, 1)

    @pl.when(jnp.logical_not(is_source))
    def _():
        pl.semaphore_wait(barrier, 7)

    @pl.when(is_source & (y_hi == 0))
    def _():
        pl.semaphore_wait(barrier, 18)

    @pl.when(is_source & (y_hi == 1))
    def _():
        pl.semaphore_wait(barrier, 19)

    n_scatter = n_sent[0]

    def scatter(top):
        k = n_scatter
        for entries in ENTRIES:
            for qy in ((2 * top + 2) % 4, (2 * top + 1) % 4, (2 * top + 3) % 4, 2 * top):
                for to_x, j in entries:
                    src, dst = chol.at[qy, pl.ds(16 * j, 16)], piece(qy, z, j)
                    if top == 0 and qy == 0 and to_x == 0:
                        yield None, pltpu.make_async_copy(src, dst, p_sem.at[j])
                    else:
                        yield remote(src, dst, p_sem.at[j], dev(to_x, qy, z, top), k), None
                        k += 1

    for top in (0, 1):

        @pl.when(is_source & (y_hi == top))
        def _():
            for away, here in scatter(top):
                (away or here).start()

    n_sent[0] = n_scatter + 24

    send(out_t, blk(p), t_sem.at[p], sib)

    def send_t_part(d, n, to):
        send(blk(p).at[pl.ds(d, n)], blk(p).at[pl.ds(d, n)], t_sem.at[p], to)

    send_t_part(0, 16, right)
    send_t_part(0, 16, left)
    for i in range(4):
        turn(i)
    send(rows_l.at[h], rows_l.at[h], l_sem, sib)

    def got(j):
        arrived(piece(y, z, j), p_sem.at[j])

    def row(xx, k):
        for j, tos in ROW_PLAN[xx]:
            quarter = piece(y, z, j)
            copies = []
            for recv, to in [(p_sem.at[j], (left, right)[t]) for t in tos] + [
                (w_sem.at[y * 4 + z], down), (w_sem.at[y * 4 + z], up), (q_sem.at[j], lo), (w_sem.at[y * 4 + z], hi)
            ]:
                copies.append(remote(quarter, quarter, recv, to, k))
                k += 1
            yield j, copies

    def row_l(xx, k):
        for j, _ in ROW_PLAN[xx]:
            quarter = piece(y_l, z, j)
            block = w_sem.at[y_l * 4 + z]
            yield j, [
                remote(quarter, quarter, recv, to, k + n)
                for n, (recv, to) in enumerate(((block, down), (u_sem.at[j], up), (block, hi)))
            ]
            k += 3

    def row_u(xx, k):
        for j, _ in ROW_PLAN[xx]:
            quarter = piece(y_l, zd, j)
            yield j, [remote(quarter, quarter, w_sem.at[y_l * 4 + zd], up, k)]
            k += 1

    n_row = n_sent[0]
    for xx in range(4):

        @pl.when(x == xx)
        def _():
            for j, copies in row(xx, n_row):
                got(j)
                for c in copies:
                    c.start()

    n_sent[0] += 22
    mine = x * 4 + y_lo * 2
    sib_p = mine + (1 - h)
    lo_p = x * 4 + (1 - y_lo) * 2 + h
    lo_s = x * 4 + (1 - y_lo) * 2 + (1 - h)
    fr = xl * 4 + y_lo * 2
    gr = xr * 4 + y_lo * 2
    fl = xr * 4 + (1 - y_lo) * 2
    gl = xl * 4 + (1 - y_lo) * 2
    wait_t(sib_p)
    for to in (right, left):
        send_t(sib_p, to)
    for to in (right, left):
        send_t_part(16, 48, to)
    send_t(p, lo)
    send_t(sib_p, lo)
    n_row_l = n_sent[0]
    for xx in range(4):

        @pl.when(x == xx)
        def _():
            for j, copies in row_l(xx, n_row_l):
                arrived(piece(y_l, z, j), q_sem.at[j])
                for c in copies:
                    c.start()

    n_sent[0] += 12
    z_pair = z + 1 - 2 * (z % 2)
    z_other = (2 * z - z_pair + 4) % 4
    wait_w(y, zd)
    wait_w(y, zu)
    send_w(y, zu, down)
    send_w(y, z_pair, hi)
    send_w(y, z_other, hi)
    n_row_u = n_sent[0]
    for xx in range(4):

        @pl.when(x == xx)
        def _():
            for j, copies in row_u(xx, n_row_u):
                arrived(piece(y_l, zd, j), u_sem.at[j])
                for c in copies:
                    c.start()

    n_sent[0] += 4
    wait_w(y_l, zu)
    arrived(rows_l.at[1 - h], l_sem)

    wide = ROW_CHUNK // 32

    def tile(zz, aa, halves=(0, 1)):
        w = win[zz, pl.ds(2 * aa, 2)].reshape(256, 2048)
        lanes = pl.ds(pl.multiple_of(zz * 128, 128), 128)
        for k in halves:
            for d0 in range(0, 64, wide):
                l = rows_l[k, pl.ds(d0, wide)].reshape(ROW_CHUNK, 2048)
                o = lax.dot_general(l, w, (((1,), (1,)), ((), ())), preferred_element_type=F32).astype(BF16)
                for q in (0, 1):
                    ints[pl.ds(d0, wide), k * 4 + 2 * aa + q, :, lanes] = o[:, q * 128 : q * 128 + 128].reshape(
                        wide, 32, 128
                    )

    zz, aa = z // 2, y // 2
    tile(zz, aa, (0,))
    wait_w(y_f, z)
    for q in (0, 1):
        half_w = wblk(y_f, z).at[pl.ds(32 * q, 32)]
        send(half_w, half_w, v_sem.at[q], down)
    send_w(y_f, z, up)
    wait_t(fr + (1 - h))
    send_t(fr + (1 - h), lo)
    send_t(fr + (1 - h), right)
    wait_t(gr + (1 - h))
    send_t(gr + (1 - h), lo)
    wait_t(lo_p)
    for to in (right, left):
        send_t(lo_p, to)
    tile(zz, aa, (1,))

    wait_t(fr + h)
    send_t(fr + h, right)
    wait_w(y, zf)
    send_w(y, zf, hi)
    wait_w(y_l, zf)

    def forward_f(q):
        half_w = wblk(y_f, zu).at[pl.ds(32 * q, 32)]
        arrived(half_w, v_sem.at[q])
        send(half_w, half_w, w_sem.at[y_f * 4 + zu], down)

    tile(1 - zz, aa, (0,))
    forward_f(0)
    tile(1 - zz, aa, (1,))
    forward_f(1)
    wait_t(fl + h)
    send_t(fl + h, left)
    away = ((x + 2) % 4) * 4
    wait_t(away + y_lo * 2 + (1 - h))
    send_t(away + y_lo * 2 + (1 - h), lo)

    wait_w(y_h, z)
    wait_w(y_h, z_pair)
    wait_w(y_f, zd)
    tile(zz, 1 - aa)
    wait_w(y_h, z_other)
    wait_w(y_f, zf)
    wait_w(y_h, zf)
    tile(1 - zz, 1 - aa)

    wait_t(lo_s)
    wait_t(gr + h)
    for k in (0, 1):
        wait_t(gl + k)
    wait_t(fl + (1 - h))
    wait_t(away + y_lo * 2 + h)
    for k in (0, 1):
        wait_t(away + (1 - y_lo) * 2 + k)

    total[...] = jnp.zeros_like(total)

    def step(i, carry):
        acc = None
        for u in range(16):
            d = i * 16 + u
            o = lax.dot_general(
                ints[d].reshape(256, 256), amps[:, d].reshape(128, 256), (((1,), (1,)), ((), ())),
                preferred_element_type=F32,
            )
            acc = o if acc is None else acc + o
        total[...] += acc
        return carry

    lax.fori_loop(0, 4, step, 0)
    turned[...] = total[...].T

    for c in started:
        c.wait_send()
    started.clear()
    for top in (0, 1):

        @pl.when(is_source & (y_hi == top))
        def _():
            for away, _ in scatter(top):
                if away is not None:
                    away.wait_send()

    for xx in range(4):

        @pl.when(x == xx)
        def _():
            for _, copies in (*row(xx, n_row), *row_l(xx, n_row_l), *row_u(xx, n_row_u)):
                for c in copies:
                    c.wait_send()

    for o in range(1, 16):
        gg, pp, i = peer(o)
        send(
            turned.at[pl.ds(pl.multiple_of(gg * 16, 16), 16), pl.ds(pl.multiple_of((i % 2) * 128, 128), 128)],
            parts.at[me], r_sem.at[me], (gg, pp),
        )
    acc = turned[pl.ds(pl.multiple_of(g * 16, 16), 16), pl.ds(pl.multiple_of(h * 128, 128), 128)]
    for o in range(15, 0, -1):
        i = peer(o)[2]
        arrived(parts.at[i], r_sem.at[i])
        acc = acc + parts[i]
    for a in range(A_WIN):
        out[a] = acc[:, a * 32 : a * 32 + 32]

    for c in started:
        c.wait_send()


def per_device(amplitudes, cholesky):
    hbm = pl.BlockSpec(memory_space=pltpu.MemorySpace.HBM)
    out = pl.pallas_call(
        kernel,
        out_shape=jax.ShapeDtypeStruct((A_WIN, 16, 32), F32),
        in_specs=[hbm] * 2,
        out_specs=pl.BlockSpec(memory_space=pltpu.VMEM),
        scratch_shapes=[
            pltpu.VMEM((32, 64, 2048), BF16),
            pltpu.VMEM((8, 64, 512), BF16),
            pltpu.VMEM((64, 8, 256), BF16),
            pltpu.VMEM((2, 64, 32, 2048), BF16),
            pltpu.VMEM((2, A_WIN, 2, 64, 2048), BF16),
            pltpu.VMEM((16, 64, 8, 256), BF16),
            pltpu.VMEM((64, 8, 32, 256), BF16),
            pltpu.VMEM((256, 128), F32),
            pltpu.VMEM((128, 256), F32),
            pltpu.VMEM((16, 16, 128), F32),
            pltpu.SemaphoreType.DMA((5,)),
            pltpu.SemaphoreType.DMA((16,)),
            pltpu.SemaphoreType.DMA((16,)),
            pltpu.SemaphoreType.DMA((4,)),
            pltpu.SemaphoreType.DMA((4,)),
            pltpu.SemaphoreType.DMA((4,)),
            pltpu.SemaphoreType.DMA((2,)),
            pltpu.SemaphoreType.DMA,
            pltpu.SemaphoreType.DMA((16,)),
            pltpu.SemaphoreType.DMA((128,)),
        ],
        compiler_params=pltpu.CompilerParams(
            collective_id=0, has_side_effects=True, vmem_limit_bytes=56 * 2**20
        ),
    )(amplitudes, cholesky)
    return out.transpose(2, 0, 1)


def solution(mesh):
    in_specs = (P("pair", "grp", None), P("pair", "grp", None))
    out_specs = P("pair", None, "grp")
    return jax.shard_map(
        per_device, mesh=mesh, in_specs=in_specs, out_specs=out_specs, check_vma=False
    )
```

```python
import jax
import jax.numpy as jnp
from jax import lax
from jax.experimental import pallas as pl
from jax.experimental.pallas import tpu as pltpu
from jax.sharding import PartitionSpec as P

A_WIN = 4
MESH = pl.DeviceIdType.MESH
F32, BF16 = jnp.float32, jnp.bfloat16


ROW_CHUNK = 1024
PEERS = tuple((dy, dz, dk) for dy in (1, 0) for dz in (2, 1, 3, 0) for dk in (1, 0))[:15]
ENTRIES = (((0, 0), (0, 2), (1, 1), (3, 3)), ((0, 1), (0, 3)))
ROW_PLAN = (
    ((0, (1, 0)), (2, (1, 0)), (1, (0,)), (3, (1,))),
    ((1, (1,)), (0, (1,)), (2, ()), (3, ())),
    ((1, ()), (3, ()), (0, ()), (2, ())),
    ((3, (0,)), (2, (0,)), (0, ()), (1, ())),
)


def kernel(
    amp, chol, out,
    raw_l, raw_t, out_t, rows_l, win, amps, ints, total, turned, parts,
    loc_sem, t_sem, w_sem, p_sem, q_sem, u_sem, v_sem, l_sem, r_sem, s_sem,
):
    g, p = lax.axis_index("grp"), lax.axis_index("pair")
    x, y_lo, h = p // 4, (p // 2) % 2, p % 2
    y_hi, z = g // 4, g % 4
    y = 2 * y_hi + y_lo
    xr, xl = (x + 1) % 4, (x + 3) % 4
    zu, zd, zf = (z + 1) % 4, (z + 3) % 4, (z + 2) % 4
    y_l = 2 * y_hi + (1 - y_lo)
    y_h = 2 * (1 - y_hi) + (1 - y_lo)
    y_f = 2 * (1 - y_hi) + y_lo

    def dev(xx, yy, zz, hh):
        return ((yy // 2) * 4 + zz, xx * 4 + (yy % 2) * 2 + hh)

    sib = dev(x, y, z, 1 - h)
    right, left = dev(xr, y, z, h), dev(xl, y, z, h)
    lo, hi = dev(x, y_l, z, h), dev(x, y_h, z, h)
    up, down = dev(x, y, zu, h), dev(x, y, zd, h)

    started = []
    n_sent = [0]

    def remote(src, dst, recv, to, k):
        return pltpu.make_async_remote_copy(
            src_ref=src, dst_ref=dst, send_sem=s_sem.at[k], recv_sem=recv, device_id=to, device_id_type=MESH
        )

    def send(src, dst, recv, to):
        c = remote(src, dst, recv, to, n_sent[0])
        n_sent[0] += 1
        c.start()
        started.append(c)

    def arrived(dst, recv):
        remote(dst, dst, recv, sib, 0).wait_recv()

    def blk(i):
        return amps.at[i]

    def wblk(a, zz):
        return win.at[zz // 2, a, zz % 2]

    def piece(a, zz, j):
        return win.at[zz // 2, a, zz % 2, pl.ds(16 * j, 16)]

    def send_t(i, to):
        send(blk(i), blk(i), t_sem.at[i], to)

    def send_w(a, zz, to):
        send(wblk(a, zz), wblk(a, zz), w_sem.at[a * 4 + zz], to)

    def wait_t(i):
        arrived(blk(i), t_sem.at[i])

    def wait_w(a, zz):
        arrived(wblk(a, zz), w_sem.at[a * 4 + zz])

    half = pl.ds(pl.multiple_of(h * 256, 256), 256)
    other = pl.ds(pl.multiple_of((1 - h) * 256, 256), 256)

    def turn(i):
        own_l[i].wait()

        def body(n, carry):
            lanes = pl.ds(pl.multiple_of(n * 256, 256), 256)
            rows_l[h, pl.ds(16 * i, 16), :, lanes] = jnp.swapaxes(raw_l[:, pl.ds(16 * i, 16), lanes], 0, 1)
            return carry

        lax.fori_loop(0, 8, body, 0)

    own_t = pltpu.make_async_copy(amp, raw_t, loc_sem.at[4])
    own_t.start()
    own_l = [
        pltpu.make_async_copy(chol.at[:, pl.ds(16 * i, 16)], raw_l.at[:, pl.ds(16 * i, 16)], loc_sem.at[i])
        for i in range(4)
    ]
    for c in own_l:
        c.start()

    barrier = pltpu.get_barrier_semaphore()

    def hello(to):
        pl.semaphore_signal(barrier, inc=1, device_id=to, device_id_type=MESH)

    me = g * 2 + h

    def peer(o):
        dy, dz, dk = PEERS[o - 1]
        gg, k = ((y_hi + dy) % 2) * 4 + (z + dz) % 4, (h + dk) % 2
        return gg, (p // 2) * 2 + k, gg * 2 + k

    for to in (sib, right, left, lo, hi, up, down):
        hello(to)
    is_source = p == 0

    @pl.when((x != 2) & jnp.logical_not(is_source & (g < 4)))
    def _():
        hello((h * 4 + z, 0))

    own_t.wait()
    amps[p] = jnp.swapaxes(raw_t[:, :, half], 0, 1)
    out_t[...] = jnp.swapaxes(raw_t[:, :, other], 0, 1)

    @pl.when(jnp.logical_not(is_source))
    def _():
        pl.semaphore_wait(barrier, 7)

    @pl.when(is_source & (y_hi == 0))
    def _():
        pl.semaphore_wait(barrier, 18)

    @pl.when(is_source & (y_hi == 1))
    def _():
        pl.semaphore_wait(barrier, 19)

    n_scatter = n_sent[0]

    def scatter(top):
        k = n_scatter
        for entries in ENTRIES:
            for qy in ((2 * top + 2) % 4, (2 * top + 1) % 4, (2 * top + 3) % 4, 2 * top):
                for to_x, j in entries:
                    src, dst = chol.at[qy, pl.ds(16 * j, 16)], piece(qy, z, j)
                    if top == 0 and qy == 0 and to_x == 0:
                        yield None, pltpu.make_async_copy(src, dst, p_sem.at[j])
                    else:
                        yield remote(src, dst, p_sem.at[j], dev(to_x, qy, z, top), k), None
                        k += 1

    for top in (0, 1):

        @pl.when(is_source & (y_hi == top))
        def _():
            for away, here in scatter(top):
                (away or here).start()

    n_sent[0] = n_scatter + 24

    send(out_t, blk(p), t_sem.at[p], sib)

    def send_t_part(d, n, to):
        send(blk(p).at[pl.ds(d, n)], blk(p).at[pl.ds(d, n)], t_sem.at[p], to)

    send_t_part(0, 16, right)
    send_t_part(0, 16, left)
    for i in range(4):
        turn(i)
    send(rows_l.at[h], rows_l.at[h], l_sem, sib)

    def got(j):
        arrived(piece(y, z, j), p_sem.at[j])

    def row(xx, k):
        for j, tos in ROW_PLAN[xx]:
            quarter = piece(y, z, j)
            copies = []
            for recv, to in [(p_sem.at[j], (left, right)[t]) for t in tos] + [
                (w_sem.at[y * 4 + z], down), (w_sem.at[y * 4 + z], up), (q_sem.at[j], lo), (w_sem.at[y * 4 + z], hi)
            ]:
                copies.append(remote(quarter, quarter, recv, to, k))
                k += 1
            yield j, copies

    def row_l(xx, k):
        for j, _ in ROW_PLAN[xx]:
            quarter = piece(y_l, z, j)
            block = w_sem.at[y_l * 4 + z]
            yield j, [
                remote(quarter, quarter, recv, to, k + n)
                for n, (recv, to) in enumerate(((block, down), (u_sem.at[j], up), (block, hi)))
            ]
            k += 3

    def row_u(xx, k):
        for j, _ in ROW_PLAN[xx]:
            quarter = piece(y_l, zd, j)
            yield j, [remote(quarter, quarter, w_sem.at[y_l * 4 + zd], up, k)]
            k += 1

    n_row = n_sent[0]
    for xx in range(4):

        @pl.when(x == xx)
        def _():
            for j, copies in row(xx, n_row):
                got(j)
                for c in copies:
                    c.start()

    n_sent[0] += 22
    mine = x * 4 + y_lo * 2
    sib_p = mine + (1 - h)
    lo_p = x * 4 + (1 - y_lo) * 2 + h
    lo_s = x * 4 + (1 - y_lo) * 2 + (1 - h)
    fr = xl * 4 + y_lo * 2
    gr = xr * 4 + y_lo * 2
    fl = xr * 4 + (1 - y_lo) * 2
    gl = xl * 4 + (1 - y_lo) * 2
    wait_t(sib_p)
    for to in (right, left):
        send_t(sib_p, to)
    for to in (right, left):
        send_t_part(16, 48, to)
    send_t(p, lo)
    send_t(sib_p, lo)
    n_row_l = n_sent[0]
    for xx in range(4):

        @pl.when(x == xx)
        def _():
            for j, copies in row_l(xx, n_row_l):
                arrived(piece(y_l, z, j), q_sem.at[j])
                for c in copies:
                    c.start()

    n_sent[0] += 12
    z_pair = z + 1 - 2 * (z % 2)
    z_other = (2 * z - z_pair + 4) % 4
    wait_w(y, zd)
    wait_w(y, zu)
    send_w(y, zu, down)
    send_w(y, z_pair, hi)
    send_w(y, z_other, hi)
    n_row_u = n_sent[0]
    for xx in range(4):

        @pl.when(x == xx)
        def _():
            for j, copies in row_u(xx, n_row_u):
                arrived(piece(y_l, zd, j), u_sem.at[j])
                for c in copies:
                    c.start()

    n_sent[0] += 4
    wait_w(y_l, zu)
    arrived(rows_l.at[1 - h], l_sem)

    wide = ROW_CHUNK // 32

    def tile(zz, aa, halves=(0, 1)):
        w = win[zz, pl.ds(2 * aa, 2)].reshape(256, 2048)
        lanes = pl.ds(pl.multiple_of(zz * 128, 128), 128)
        for k in halves:
            for d0 in range(0, 64, wide):
                l = rows_l[k, pl.ds(d0, wide)].reshape(ROW_CHUNK, 2048)
                o = lax.dot_general(l, w, (((1,), (1,)), ((), ())), preferred_element_type=F32).astype(BF16)
                for q in (0, 1):
                    ints[pl.ds(d0, wide), k * 4 + 2 * aa + q, :, lanes] = o[:, q * 128 : q * 128 + 128].reshape(
                        wide, 32, 128
                    )

    zz, aa = z // 2, y // 2
    tile(zz, aa, (0,))
    wait_w(y_f, z)
    for q in (0, 1):
        half_w = wblk(y_f, z).at[pl.ds(32 * q, 32)]
        send(half_w, half_w, v_sem.at[q], down)
    send_w(y_f, z, up)
    wait_t(fr + (1 - h))
    send_t(fr + (1 - h), lo)
    send_t(fr + (1 - h), right)
    wait_t(gr + (1 - h))
    send_t(gr + (1 - h), lo)
    wait_t(lo_p)
    for to in (right, left):
        send_t(lo_p, to)
    tile(zz, aa, (1,))

    wait_t(fr + h)
    send_t(fr + h, right)
    wait_w(y, zf)
    send_w(y, zf, hi)
    wait_w(y_l, zf)

    def forward_f(q):
        half_w = wblk(y_f, zu).at[pl.ds(32 * q, 32)]
        arrived(half_w, v_sem.at[q])
        send(half_w, half_w, w_sem.at[y_f * 4 + zu], down)

    tile(1 - zz, aa, (0,))
    forward_f(0)
    tile(1 - zz, aa, (1,))
    forward_f(1)
    wait_t(fl + h)
    send_t(fl + h, left)

    wait_w(y_h, z)
    wait_w(y_h, z_pair)
    wait_w(y_f, zd)
    tile(zz, 1 - aa, (0,))
    away = ((x + 2) % 4) * 4
    wait_t(away + y_lo * 2 + (1 - h))
    send_t(away + y_lo * 2 + (1 - h), lo)
    tile(zz, 1 - aa, (1,))
    wait_w(y_h, z_other)
    wait_w(y_f, zf)
    wait_w(y_h, zf)
    tile(1 - zz, 1 - aa)

    wait_t(lo_s)
    wait_t(gr + h)
    for k in (0, 1):
        wait_t(gl + k)
    wait_t(fl + (1 - h))
    wait_t(away + y_lo * 2 + h)
    for k in (0, 1):
        wait_t(away + (1 - y_lo) * 2 + k)

    total[...] = jnp.zeros_like(total)

    def step(i, carry):
        acc = None
        for u in range(16):
            d = i * 16 + u
            o = lax.dot_general(
                ints[d].reshape(256, 256), amps[:, d].reshape(128, 256), (((1,), (1,)), ((), ())),
                preferred_element_type=F32,
            )
            acc = o if acc is None else acc + o
        total[...] += acc
        return carry

    lax.fori_loop(0, 4, step, 0)
    turned[...] = total[...].T

    for c in started:
        c.wait_send()
    started.clear()
    for top in (0, 1):

        @pl.when(is_source & (y_hi == top))
        def _():
            for away, _ in scatter(top):
                if away is not None:
                    away.wait_send()

    for xx in range(4):

        @pl.when(x == xx)
        def _():
            for _, copies in (*row(xx, n_row), *row_l(xx, n_row_l), *row_u(xx, n_row_u)):
                for c in copies:
                    c.wait_send()

    for o in range(1, 16):
        gg, pp, i = peer(o)
        send(
            turned.at[pl.ds(pl.multiple_of(gg * 16, 16), 16), pl.ds(pl.multiple_of((i % 2) * 128, 128), 128)],
            parts.at[me], r_sem.at[me], (gg, pp),
        )
    acc = turned[pl.ds(pl.multiple_of(g * 16, 16), 16), pl.ds(pl.multiple_of(h * 128, 128), 128)]
    for o in range(15, 0, -1):
        i = peer(o)[2]
        arrived(parts.at[i], r_sem.at[i])
        acc = acc + parts[i]
    for a in range(A_WIN):
        out[a] = acc[:, a * 32 : a * 32 + 32]

    for c in started:
        c.wait_send()


def per_device(amplitudes, cholesky):
    hbm = pl.BlockSpec(memory_space=pltpu.MemorySpace.HBM)
    out = pl.pallas_call(
        kernel,
        out_shape=jax.ShapeDtypeStruct((A_WIN, 16, 32), F32),
        in_specs=[hbm] * 2,
        out_specs=pl.BlockSpec(memory_space=pltpu.VMEM),
        scratch_shapes=[
            pltpu.VMEM((32, 64, 2048), BF16),
            pltpu.VMEM((8, 64, 512), BF16),
            pltpu.VMEM((64, 8, 256), BF16),
            pltpu.VMEM((2, 64, 32, 2048), BF16),
            pltpu.VMEM((2, A_WIN, 2, 64, 2048), BF16),
            pltpu.VMEM((16, 64, 8, 256), BF16),
            pltpu.VMEM((64, 8, 32, 256), BF16),
            pltpu.VMEM((256, 128), F32),
            pltpu.VMEM((128, 256), F32),
            pltpu.VMEM((16, 16, 128), F32),
            pltpu.SemaphoreType.DMA((5,)),
            pltpu.SemaphoreType.DMA((16,)),
            pltpu.SemaphoreType.DMA((16,)),
            pltpu.SemaphoreType.DMA((4,)),
            pltpu.SemaphoreType.DMA((4,)),
            pltpu.SemaphoreType.DMA((4,)),
            pltpu.SemaphoreType.DMA((2,)),
            pltpu.SemaphoreType.DMA,
            pltpu.SemaphoreType.DMA((16,)),
            pltpu.SemaphoreType.DMA((128,)),
        ],
        compiler_params=pltpu.CompilerParams(
            collective_id=0, has_side_effects=True, vmem_limit_bytes=56 * 2**20
        ),
    )(amplitudes, cholesky)
    return out.transpose(2, 0, 1)


def solution(mesh):
    in_specs = (P("pair", "grp", None), P("pair", "grp", None))
    out_specs = P("pair", None, "grp")
    return jax.shard_map(
        per_device, mesh=mesh, in_specs=in_specs, out_specs=out_specs, check_vma=False
    )
```
